32 devices in a mesh: part: 1 (over z), row: 4 (over y), col: 8 (over x, core).
Axes of the slice: x: 4, y: 4, z: 1, core: 2. Of those that a mesh axis runs over, the one named last changes fastest.
The devices are a block of a 4x4x8 slice.
Arguments:
- counts: bfloat16 [16384, 8192], P(('part', 'row'), 'col')
- w_init: float32 [16384, 1024], P(('part', 'row'))
- h_init: float32 [1024, 8192], P(None, ('part', 'col'))
Outputs:
- output 1: float32 [16384, 1024], P(('part', 'row'))
- output 2: float32 [1024, 8192], P(None, ('part', 'col'))
All inputs are finite; a program needn't handle non-finite values.
Results may differ from the reference program's by a relative error of at most 0.001.
Values are sent between devices in bfloat16 or wider.
A program may use at most 768 MiB of HBM per device.

```python
import jax
import jax.numpy as jnp
from jax import lax

ROW_DEVS = 4
COL_DEVS = 8
DOC_DEV = 4096
WORD_DEV = 1024
TOPICS = 1024
SWEEPS = 4
LATENT = 8

DOCS = ROW_DEVS * DOC_DEV
WORDS = COL_DEVS * WORD_DEV
EPS = 1e-6


def setup_inputs(seed: int = 0, part: int = 0) -> dict:
    base_key = jax.random.fold_in(jax.random.key(seed), part)
    sub_keys = jax.random.split(base_key, 7)
    w_true = jax.random.randint(sub_keys[0], (DOCS, LATENT), 0, 4)
    h_true = jax.random.randint(sub_keys[1], (LATENT, WORDS), 0, 4)
    noise_int = jax.random.randint(sub_keys[2], (DOCS, WORDS), -3, 4)
    counts = jnp.clip(jnp.dot(w_true, h_true) + noise_int, 0, 256).astype(jnp.bfloat16)
    init_scale = 4.0 * TOPICS ** -0.5
    w_gain = 2.0 ** jax.random.uniform(sub_keys[3], (1, TOPICS), jnp.float32, -1.0, 1.0)
    h_gain = 2.0 ** jax.random.uniform(sub_keys[4], (TOPICS, 1), jnp.float32, -1.0, 1.0)
    w_init = jax.random.uniform(sub_keys[5], (DOCS, TOPICS), jnp.float32, 0.5, 1.5) * w_gain * init_scale
    h_init = jax.random.uniform(sub_keys[6], (TOPICS, WORDS), jnp.float32, 0.5, 1.5) * h_gain * init_scale
    return {'counts': counts, 'w_init': w_init.astype(jnp.float32), 'h_init': h_init.astype(jnp.float32)}


def ratio_block(c_blk, w_blk, h_blk):
    z_blk = jnp.dot(w_blk, h_blk, preferred_element_type=jnp.float32)
    return (c_blk.astype(jnp.float32) / (z_blk + EPS)).astype(jnp.bfloat16)


def update_w(w_cur, h_cur, c_by_row):
    w_blocks = w_cur.astype(jnp.bfloat16).reshape(ROW_DEVS, DOC_DEV, TOPICS)
    h_blocks = h_cur.astype(jnp.bfloat16).reshape(TOPICS, COL_DEVS, WORD_DEV).transpose(1, 0, 2)

    def one_row(row_items):
        w_blk, c_row = row_items

        def col_step(running, col_items):
            h_blk, c_blk = col_items
            q_blk = ratio_block(c_blk, w_blk, h_blk)
            return running + jnp.dot(q_blk, h_blk.T, preferred_element_type=jnp.float32), None

        total, _ = lax.scan(col_step, jnp.zeros((DOC_DEV, TOPICS), jnp.float32), (h_blocks, c_row))
        return total

    a_w = lax.map(one_row, (w_blocks, c_by_row)).reshape(DOCS, TOPICS)
    s_h = jnp.sum(h_cur, axis=1)
    return w_cur * a_w / s_h[None, :]


def update_h(w_cur, h_cur, c_by_col):
    w_blocks = w_cur.astype(jnp.bfloat16).reshape(ROW_DEVS, DOC_DEV, TOPICS)
    h_blocks = h_cur.astype(jnp.bfloat16).reshape(TOPICS, COL_DEVS, WORD_DEV).transpose(1, 0, 2)

    def one_col(col_items):
        h_blk, c_col = col_items

        def row_step(running, row_items):
            w_blk, c_blk = row_items
            q_blk = ratio_block(c_blk, w_blk, h_blk)
            return running + jnp.dot(w_blk.T, q_blk, preferred_element_type=jnp.float32), None

        total, _ = lax.scan(row_step, jnp.zeros((TOPICS, WORD_DEV), jnp.float32), (w_blocks, c_col))
        return total

    a_h = lax.map(one_col, (h_blocks, c_by_col)).transpose(1, 0, 2).reshape(TOPICS, WORDS)
    s_w = jnp.sum(w_cur, axis=0)
    return h_cur * a_h / s_w[:, None]


def reference(counts, w_init, h_init):
    c_blocks = counts.reshape(ROW_DEVS, DOC_DEV, COL_DEVS, WORD_DEV)
    c_by_row = c_blocks.transpose(0, 2, 1, 3)
    c_by_col = c_blocks.transpose(2, 0, 1, 3)

    def one_sweep(state, unused):
        w_cur, h_cur = state
        w_cur = update_w(w_cur, h_cur, c_by_row)
        h_cur = update_h(w_cur, h_cur, c_by_col)
        return (w_cur, h_cur), None

    (w_out, h_out), _ = lax.scan(one_sweep, (w_init, h_init), None, length=SWEEPS)
    return (w_out, h_out)
```

```python
import functools

import jax
import jax.numpy as jnp
from jax import lax
from jax.experimental import pallas as pl
from jax.experimental.pallas import tpu as pltpu
from jax.sharding import PartitionSpec as P

SWEEPS = 4
EPS = 1e-6
RING = 4
SUBS = 2
BLK = 512
EW = 32
MESH = pl.DeviceIdType.MESH
F32 = jnp.float32
BF = jnp.bfloat16
CONTRACT_LAST = (((1,), (1,)), ((), ()))
CONTRACT_FIRST = (((0,), (0,)), ((), ()))


def mult(v, m):
    return pl.multiple_of(v, m)


def kernel(c_hbm, wb_hbm, hb_hbm, w0_hbm, h0_hbm, w_out, h_out,
           cv, wb, hb, wf, hf, wacc, hacc, wring, hring, wst, hst, d2d, sbuf, srecv, sfin,
           ld_sem, wr_s, wr_r, hr_s, hr_r, d2_s, d2_r, ag_s, ag_r, pg_s, pg_r, ss_s, ss_r):
    col = lax.axis_index("col")
    y = lax.axis_index("row")
    x, c = col // 2, lax.rem(col, 2)
    d = 1 - 2 * c
    docs, topics = wb.shape
    words = hb.shape[0]
    sw = docs // (2 * RING)
    sh = words // RING

    def mod(v):
        return lax.rem(v + 4 * RING, RING)

    def xdev(delta):
        return {"col": mod(x + delta) * 2 + c}

    def ydev(delta):
        return {"row": mod(y + delta)}

    partner = {"col": x * 2 + (1 - c)}

    def remote(src, dst, s_sem, r_sem, dev):
        return pltpu.make_async_remote_copy(src_ref=src, dst_ref=dst, send_sem=s_sem, recv_sem=r_sem,
                                            device_id=dev, device_id_type=MESH)

    barrier = pltpu.get_barrier_semaphore()
    for o in range(1, RING):
        pl.semaphore_signal(barrier, inc=1, device_id=xdev(o), device_id_type=MESH)
        pl.semaphore_signal(barrier, inc=1, device_id=ydev(o), device_id_type=MESH)
    pl.semaphore_signal(barrier, inc=1, device_id=partner, device_id_type=MESH)

    def wrows(k, h):
        return pl.ds(mult((k * 2 + h) * sw, sw), sw)

    def hrows(k):
        return pl.ds(mult(k * sh, sh), sh)

    loads = [
        pltpu.make_async_copy(hb_hbm, hb, ld_sem.at[0]),
        pltpu.make_async_copy(wb_hbm, wb, ld_sem.at[1]),
        pltpu.make_async_copy(c_hbm, cv, ld_sem.at[2]),
        pltpu.make_async_copy(w0_hbm.at[wrows(x, c)], wf, ld_sem.at[3]),
        pltpu.make_async_copy(h0_hbm.at[hrows(y)], hf, ld_sem.at[4]),
    ]
    for cp in loads:
        cp.start()
    pl.semaphore_wait(barrier, 2 * (RING - 1) + 1)
    for cp in loads:
        cp.wait()

    class Gather:
        def __init__(self, buf, own, slot, is_w):
            self.buf, self.own, self.slot, self.is_w = buf, own, slot, is_w
            self.p = x if is_w else y
            self.dev = xdev if is_w else ydev

        def rows(self, k, h):
            return wrows(k, h) if self.is_w else hrows(k)

        def ring(self, i):
            k = self.p if i < 2 else mod(self.p - d)
            dst = self.buf.at[self.rows(k, c)]
            src = self.own if (i < 2 and self.own is not None) else dst
            return remote(src, dst, ag_s.at[self.slot, i], ag_r.at[self.slot, i], self.dev(-d if i == 1 else d))

        def ring_in(self, i):
            k = mod(self.p + (-d, d, -2 * d)[i])
            dst = self.buf.at[self.rows(k, c)]
            return remote(dst, dst, ag_s.at[self.slot, i], ag_r.at[self.slot, i], self.dev(d))

        def pair(self, i):
            k = mod(self.p + (0, -d, d, 2)[i])
            dst = self.buf.at[self.rows(k, c)]
            src = self.own if (i == 0 and self.own is not None) else dst
            return remote(src, dst, pg_s.at[self.slot, i], pg_r.at[self.slot, i], partner)

        def pair_in(self, i):
            k = mod(self.p + (0, d, -d, 2)[i])
            dst = self.buf.at[self.rows(k, 1 - c)]
            return remote(dst, dst, pg_s.at[self.slot, i], pg_r.at[self.slot, i], partner)

        def start(self):
            self.ring(0).start()
            self.ring(1).start()
            if self.is_w:
                self.pair(0).start()

        def got(self, i):
            self.ring_in(i).wait_recv()
            if i == 0:
                self.ring(2).start()
            if self.is_w:
                self.pair(i + 1).start()

        def got_pair(self, i):
            if self.is_w:
                self.pair_in(i).wait_recv()

        def sent(self):
            for i in range(3):
                self.ring(i).wait_send()
            if self.is_w:
                for i in range(4):
                    self.pair(i).wait_send()

    wag = Gather(wb, None, 0, True)
    hag = Gather(hb, None, 1, False)
    wfin = Gather(w_out, wf, 2, True)
    hfin = Gather(h_out, hf, 3, False)

    class Sums:
        def __init__(self, role):
            self.r = role

        def copies(self, stage):
            r = self.r
            if stage == 0:
                return [remote(sbuf.at[r, 0], srecv.at[r, 0], ss_s.at[r, 0], ss_r.at[r, 0], partner)]
            dev = xdev if stage == 1 else ydev
            base = 1 if stage == 1 else RING
            return [remote(sbuf.at[r, stage], srecv.at[r, base + o - 1], ss_s.at[r, base + o - 1],
                           ss_r.at[r, base + o - 1], dev(o)) for o in range(1, RING)]

        def start(self, value):
            sbuf[self.r, 0] = value
            for cp in self.copies(0):
                cp.start()

        def step(self, stage):
            r = self.r
            cps = self.copies(stage - 1)
            total = sbuf[r, stage - 1]
            base = (0, 1, RING)[stage - 1]
            for i, cp in enumerate(cps):
                cp.wait_recv()
                total = total + srecv[r, base + i]
            for cp in cps:
                cp.wait_send()
            if stage < 3:
                sbuf[r, stage] = total
                for cp in self.copies(stage):
                    cp.start()
            else:
                sfin[r] = jnp.broadcast_to(jnp.sum(total, axis=0, keepdims=True), (8, topics))

    wsum, hsum = Sums(0), Sums(1)

    def colsum(ref):
        n = ref.shape[0]

        def body(i, tot):
            return tot + ref[pl.ds(mult(i * 8, 8), 8), :]

        return lax.fori_loop(0, n // 8, body, jnp.zeros((8, topics), F32), unroll=4)

    def w_part(rows, kk, width, first, dst_rows):
        cols = pl.ds(mult(kk * width, width), width)
        hk = hb[cols, :]
        z = lax.dot_general(wb[rows, :], hk, CONTRACT_LAST, preferred_element_type=F32)
        q = (cv[rows, cols].astype(F32) / (z + EPS)).astype(BF)
        a = jnp.dot(q, hk, preferred_element_type=F32)
        if first:
            wacc[dst_rows, :] = a
        else:
            wacc[dst_rows, :] += a

    def w_unit(s, kk, width, first):
        ko, kp = mod(x - (1 + s) * d), mod(x + (1 + s) * d)
        r_own, r_par = (ko * 2 + c) * sw, (kp * 2 + 1 - c) * sw
        per = sw // BLK

        @pl.loop(0, 2 * per)
        def _(i):
            base = jnp.where(i < per, r_own, r_par - sw)
            w_part(pl.ds(mult(base + i * BLK, BLK), BLK), kk, width, first, pl.ds(mult(i * BLK, BLK), BLK))

    def h_part(docs0, words_k, acc, first):
        rows = pl.ds(mult(docs0, BLK), BLK)
        cols = hrows(words_k)
        z = lax.dot_general(wb[rows, :], hb[cols, :], CONTRACT_LAST, preferred_element_type=F32)
        q = (cv[rows, cols].astype(F32) / (z + EPS)).astype(BF)
        a = lax.dot_general(q, wb[rows, :], CONTRACT_FIRST, preferred_element_type=F32)
        if first:
            acc[...] = a
        else:
            acc[...] += a

    def ring_out(ring, stage, s, i, rows_n, s_sem, r_sem, dev, from_stage):
        n = rows_n // SUBS
        rows = pl.ds(i * n, n)
        src = stage.at[rows] if from_stage else ring.at[s - 1, rows]
        return remote(src, ring.at[s, rows], s_sem.at[s, i], r_sem.at[s, i], dev)

    def d2d_copy(s):
        slot = lax.rem(s, 2)
        return remote(wacc.at[pl.ds(sw, sw)], d2d.at[slot], d2_s.at[slot], d2_r.at[slot], partner)

    def w_sweep(t):
        dev = xdev(d)
        p = y
        order = (p, mod(p - d), mod(p + d), mod(p + 2))
        w_unit(0, order[0], sh, True)

        @pl.when(t > 0)
        def _():
            hag.got(0)
            hag.got(1)

        hsum.step(1)
        w_unit(0, order[1], sh, False)
        w_unit(0, order[2], sh, False)
        hsum.step(2)

        @pl.when(t > 0)
        def _():
            hag.got(2)

        w_unit(0, order[3], sh, False)

        @pl.when(t > 0)
        def _():
            hag.sent()

        d2d_copy(0).start()
        d2d_copy(0).wait_recv()
        n = sw // SUBS
        for i in range(SUBS):
            @pl.loop(0, n // EW)
            def _(b):
                rows = pl.ds(mult(i * n + b * EW, EW), EW)
                wst[rows, :] = wacc[rows, :] + d2d[0, rows, :]
            ring_out(wring, wst, 0, i, sw, wr_s, wr_r, dev, True).start()
        hsum.step(3)
        d2d_copy(0).wait_send()

        @pl.loop(1, RING - 1)
        def _(s):
            w_unit(s, 0, words, True)
            d2d_copy(s).start()
            d2d_copy(s).wait_recv()
            slot = lax.rem(s, 2)
            for i in range(SUBS):
                ring_out(wring, wst, s - 1, i, sw, wr_s, wr_r, dev, True).wait_recv()

                @pl.loop(0, n // EW)
                def _(b):
                    rows = pl.ds(mult(i * n + b * EW, EW), EW)
                    wring[s - 1, rows, :] = wring[s - 1, rows, :] + (wacc[rows, :] + d2d[slot, rows, :])
                ring_out(wring, wst, s, i, sw, wr_s, wr_r, dev, False).start()
            d2d_copy(s).wait_send()

        s = RING - 1
        w_unit(s, 0, words, True)
        d2d_copy(s).start()
        d2d_copy(s).wait_recv()
        own = (x * 2 + c) * sw
        tot = jnp.zeros((8, topics), F32)
        for i in range(SUBS):
            ring_out(wring, wst, s - 1, i, sw, wr_s, wr_r, dev, False).wait_recv()

            def body(b, tot):
                r0 = mult(i * n + b * 16, 16)
                rows = pl.ds(r0, 16)
                a = wring[s - 1, rows, :] + (wacc[rows, :] + d2d[s % 2, rows, :])
                new = wf[rows, :] * a / jnp.concatenate([sfin[1], sfin[1]], axis=0)
                wf[rows, :] = new
                wb[pl.ds(mult(own + r0, 16), 16), :] = new.astype(BF)
                return tot + (new[:8] + new[8:])
            tot = lax.fori_loop(0, n // 16, body, tot)
        for ss in range(RING - 1):
            for i in range(SUBS):
                ring_out(wring, wst, ss, i, sw, wr_s, wr_r, dev, ss == 0).wait_send()
        d2d_copy(s).wait_send()
        wag.start()
        wsum.start(tot)

    def h_chunk(k, words_k, acc, first):
        per = 2 * sw // BLK
        base = k * 2 * sw
        if first:
            h_part(base, words_k, acc, True)

        @pl.loop(1 if first else 0, per)
        def _(i):
            h_part(base + i * BLK, words_k, acc, False)

    def h_sweep(t):
        dev = ydev(d)
        k0 = mod(y - d)
        n = sh // SUBS
        wag.got_pair(0)
        h_chunk(x, k0, hst, True)
        wsum.step(1)
        wag.got(0)
        wag.got(1)
        wag.got_pair(2)
        h_chunk(mod(x - d), k0, hst, False)
        wag.got_pair(1)
        h_chunk(mod(x + d), k0, hst, False)
        wsum.step(2)
        wag.got(2)
        wag.got_pair(3)
        h_chunk(mod(x + 2), k0, hst, False)
        wag.sent()
        for i in range(SUBS):
            ring_out(hring, hst, 0, i, sh, hr_s, hr_r, dev, True).start()

        @pl.when(t == SWEEPS - 1)
        def _():
            wfin.start()
            pltpu.make_async_copy(wf, w_out.at[wrows(x, c)], ld_sem.at[0]).start()

        wsum.step(3)

        @pl.loop(1, RING - 1)
        def _(s):
            k = mod(y - (1 + s) * d)
            h_part(0, k, hacc, True)

            @pl.loop(1, docs // BLK)
            def _(b):
                h_part(b * BLK, k, hacc, False)
            for i in range(SUBS):
                ring_out(hring, hst, s - 1, i, sh, hr_s, hr_r, dev, True).wait_recv()

                @pl.loop(0, n // EW)
                def _(b):
                    rows = pl.ds(mult(i * n + b * EW, EW), EW)
                    hring[s - 1, rows, :] = hring[s - 1, rows, :] + hacc[rows, :]
                ring_out(hring, hst, s, i, sh, hr_s, hr_r, dev, False).start()

        s = RING - 1
        h_part(0, y, hacc, True)

        @pl.loop(1, docs // BLK)
        def _(b):
            h_part(b * BLK, y, hacc, False)
        tot = jnp.zeros((8, topics), F32)
        for i in range(SUBS):
            ring_out(hring, hst, s - 1, i, sh, hr_s, hr_r, dev, False).wait_recv()

            def body(b, tot):
                r0 = mult(i * n + b * 16, 16)
                rows = pl.ds(r0, 16)
                a = hring[s - 1, rows, :] + hacc[rows, :]
                new = hf[rows, :] * a / jnp.concatenate([sfin[0], sfin[0]], axis=0)
                hf[rows, :] = new
                hb[pl.ds(mult(y * sh + r0, 16), 16), :] = new.astype(BF)
                return tot + (new[:8] + new[8:])
            tot = lax.fori_loop(0, n // 16, body, tot)
        for ss in range(RING - 1):
            for i in range(SUBS):
                ring_out(hring, hst, ss, i, sh, hr_s, hr_r, dev, ss == 0).wait_send()

        @pl.when(t < SWEEPS - 1)
        def _():
            hag.start()
            hsum.start(tot)

    hsum.start(colsum(hf))

    @pl.loop(0, SWEEPS)
    def _(t):
        w_sweep(t)
        h_sweep(t)

    hfin.start()
    hlocal = pltpu.make_async_copy(hf, h_out.at[hrows(y)], ld_sem.at[1])
    hlocal.start()
    wfin.got(0)
    wfin.got(1)
    hfin.got(0)
    hfin.got(1)
    wfin.got(2)
    hfin.got(2)
    for i in range(4):
        wfin.got_pair(i)
    wfin.sent()
    hfin.sent()
    hlocal.wait()
    pltpu.make_async_copy(wf, w_out.at[wrows(x, c)], ld_sem.at[0]).wait()


def local(c_blk, w_loc, h_loc):
    docs, words = c_blk.shape
    topics = w_loc.shape[1]
    ht = h_loc.T
    sw, sh = docs // (2 * RING), words // RING
    dma = pltpu.SemaphoreType.DMA
    w_out, h_out = pl.pallas_call(
        kernel,
        out_shape=(jax.ShapeDtypeStruct((docs, topics), F32), jax.ShapeDtypeStruct((words, topics), F32)),
        in_specs=[pl.BlockSpec(memory_space=pl.ANY)] * 5,
        out_specs=(pl.BlockSpec(memory_space=pl.ANY), pl.BlockSpec(memory_space=pl.ANY)),
        scratch_shapes=[
            pltpu.VMEM((docs, words), BF),
            pltpu.VMEM((docs, topics), BF),
            pltpu.VMEM((words, topics), BF),
            pltpu.VMEM((sw, topics), F32),
            pltpu.VMEM((sh, topics), F32),
            pltpu.VMEM((2 * sw, topics), F32),
            pltpu.VMEM((sh, topics), F32),
            pltpu.VMEM((RING - 1, sw, topics), F32),
            pltpu.VMEM((RING - 1, sh, topics), F32),
            pltpu.VMEM((sw, topics), F32),
            pltpu.VMEM((sh, topics), F32),
            pltpu.VMEM((2, sw, topics), F32),
            pltpu.VMEM((2, 3, 8, topics), F32),
            pltpu.VMEM((2, 2 * RING - 1, 8, topics), F32),
            pltpu.VMEM((2, 8, topics), F32),
            dma((5,)),
            dma((RING - 1, SUBS)), dma((RING - 1, SUBS)),
            dma((RING - 1, SUBS)), dma((RING - 1, SUBS)),
            dma((2,)), dma((2,)),
            dma((4, 3)), dma((4, 3)),
            dma((4, 4)), dma((4, 4)),
            dma((2, 2 * RING - 1)), dma((2, 2 * RING - 1)),
        ],
        compiler_params=pltpu.CompilerParams(collective_id=0, has_side_effects=True,
                                             vmem_limit_bytes=63 * 1024 * 1024),
    )(c_blk, w_loc.astype(BF), ht.astype(BF), w_loc, ht)
    return w_out, h_out.T


def solution(mesh):
    spec_c = P(('part', 'row'), 'col')
    spec_w = P(('part', 'row'), None)
    spec_h = P(None, ('part', 'col'))
    return jax.shard_map(local, mesh=mesh, in_specs=(spec_c, spec_w, spec_h), out_specs=(spec_w, spec_h), check_vma=False)
```

```python
import functools

import jax
import jax.numpy as jnp
from jax import lax
from jax.experimental import pallas as pl
from jax.experimental.pallas import tpu as pltpu
from jax.sharding import PartitionSpec as P

SWEEPS = 4
EPS = 1e-6
RING = 4
SUBS = 2
BLK = 512
EW = 32
ORDER = ((1, 0), (3, 0), (0, 1), (0, 3), (1, 1), (3, 3), (1, 3), (3, 1),
         (2, 0), (0, 2), (2, 1), (1, 2), (2, 3), (3, 2), (2, 2))
MESH = pl.DeviceIdType.MESH
F32 = jnp.float32
BF = jnp.bfloat16
CONTRACT_LAST = (((1,), (1,)), ((), ()))
CONTRACT_FIRST = (((0,), (0,)), ((), ()))


def mult(v, m):
    return pl.multiple_of(v, m)


def kernel(c_hbm, w0_hbm, h0_hbm, w_out, h_out,
           cv, wb, hb, wf, hf, wacc, hacc, wring, hring, wst, hst, d2d, sbuf, srecv, sfin,
           ld_sem, c_s, c_r, wr_s, wr_r, hr_s, hr_r, d2_s, d2_r, ag_s, ag_r, pg_s, pg_r, ss_s, ss_r):
    col = lax.axis_index("col")
    y = lax.axis_index("row")
    x, c = col // 2, lax.rem(col, 2)
    d = 1 - 2 * c
    _, docs, topics = wb.shape
    words = hb.shape[1]
    sw = docs // (2 * RING)
    sh = words // RING

    def mod(v):
        return lax.rem(v + 4 * RING, RING)

    def xdev(delta):
        return {"col": mod(x + delta) * 2 + c}

    def ydev(delta):
        return {"row": mod(y + delta)}

    def xydev(dx, dy):
        return {"row": mod(y + dy), "col": mod(x + dx) * 2 + c}

    partner = {"col": x * 2 + (1 - c)}
    wpos, hpos = (x, y), (y, x)
    wdev, hdev = (xdev, ydev), (ydev, xdev)

    def remote(src, dst, s_sem, r_sem, dev):
        return pltpu.make_async_remote_copy(src_ref=src, dst_ref=dst, send_sem=s_sem, recv_sem=r_sem,
                                            device_id=dev, device_id_type=MESH)

    barrier = pltpu.get_barrier_semaphore()
    for dx, dy in ORDER:
        pl.semaphore_signal(barrier, inc=1, device_id=xydev(dx, dy), device_id_type=MESH)
    pl.semaphore_signal(barrier, inc=1, device_id=partner, device_id_type=MESH)

    def wrows(k, h, base=0):
        return pl.ds(mult((k * 2 + h) * sw + base, sw), sw)

    def hrows(k):
        return pl.ds(mult(k * sh, sh), sh)

    def crows(k, base=0):
        return pl.ds(mult(k * 2 * sw + base, 2 * sw), 2 * sw)

    def hblock(b):
        return hring.at[b // (RING - 1), b % (RING - 1)]

    def wload(b):
        return pltpu.make_async_copy(w0_hbm.at[crows(b)], wacc.at[b % 2], ld_sem.at[9 + b])

    loads = [
        pltpu.make_async_copy(w0_hbm.at[wrows(x, c, docs)], wf.at[1], ld_sem.at[0]),
        pltpu.make_async_copy(w0_hbm.at[wrows(x, c)], wf.at[0], ld_sem.at[1]),
        pltpu.make_async_copy(c_hbm.at[pl.ds(0, docs)], cv.at[0], ld_sem.at[2]),
        pltpu.make_async_copy(c_hbm.at[crows(x, docs), hrows(y)], cv.at[1, crows(y), hrows(x)], ld_sem.at[3]),
    ]
    hloads = [pltpu.make_async_copy(h0_hbm.at[hrows(b)], hblock(b), ld_sem.at[4 + b]) for b in range(topics // sh)]
    for cp in hloads + loads + [wload(0), wload(1)]:
        cp.start()

    def c_move(dx, dy):
        return remote(c_hbm.at[crows(mod(x + dx), docs), hrows(mod(y + dy))], cv.at[1, crows(y), hrows(x)],
                      c_s.at[dx, dy], c_r.at[dx, dy], xydev(dx, dy))

    def c_in(dx, dy):
        dst = cv.at[1, crows(mod(y - dy)), hrows(mod(x - dx))]
        return remote(dst, dst, c_s.at[dx, dy], c_r.at[dx, dy], xydev(dx, dy))

    def piece(rows, j):
        n = rows.size // SUBS
        return pl.ds(mult(rows.start + j * n, n), n)

    class Gather:
        def __init__(self, buf, own, slot, pos, dev, rows, is_w):
            self.buf, self.own, self.slot, self.is_w = buf, own, slot, is_w
            self.p, self.dev, self.rows = pos, dev, rows

        def make(self, k, h, j, own, s_sem, r_sem, i, dev):
            rows = self.rows(k, h)
            dst = self.buf.at[piece(rows, j)]
            src = dst
            if own and self.own is not None:
                n = rows.size // SUBS
                src = self.own.at[pl.ds(j * n, n)]
            return remote(src, dst, s_sem.at[self.slot, i, j], r_sem.at[self.slot, i, j], dev)

        def ring(self, i, j):
            k = self.p if i < 2 else mod(self.p - d)
            return self.make(k, c, j, i < 2, ag_s, ag_r, i, self.dev(-d if i == 1 else d))

        def ring_in(self, i, j):
            k = mod(self.p + (-d, d, -2 * d)[i])
            return self.make(k, c, j, False, ag_s, ag_r, i, self.dev(d))

        def pair(self, i, j):
            k = mod(self.p + (0, -d, d, 2)[i])
            return self.make(k, c, j, i == 0, pg_s, pg_r, i, partner)

        def pair_in(self, i, j):
            k = mod(self.p + (0, d, -d, 2)[i])
            return self.make(k, 1 - c, j, False, pg_s, pg_r, i, partner)

        def start(self, j):
            self.ring(0, j).start()
            self.ring(1, j).start()
            if self.is_w:
                self.pair(0, j).start()

        def got(self, i, j):
            self.ring_in(i, j).wait_recv()
            if i == 0:
                self.ring(2, j).start()
            if self.is_w:
                self.pair(i + 1, j).start()

        def got_pair(self, i):
            if self.is_w:
                for j in range(SUBS):
                    self.pair_in(i, j).wait_recv()

        def sent(self):
            for j in range(SUBS):
                for i in range(3):
                    self.ring(i, j).wait_send()
                if self.is_w:
                    for i in range(4):
                        self.pair(i, j).wait_send()

    def got_near(gathers):
        for j in range(SUBS):
            for i in range(2):
                for ga in gathers:
                    ga.got(i, j)

    def got_far(gathers):
        for j in range(SUBS):
            for ga in gathers:
                ga.got(2, j)

    wag = [Gather(wb.at[g], None, g, wpos[g], wdev[g], wrows, True) for g in range(2)]
    hag = [Gather(hb.at[g], None, 2 + g, hpos[g], hdev[g], lambda k, h: hrows(k), False) for g in range(2)]
    wfin = [Gather(w_out, wf.at[g], 4 + g, x, xdev, functools.partial(wrows, base=g * docs), True) for g in range(2)]
    hfin = Gather(h_out, hf, 6, y, ydev, lambda k, h: hrows(k), False)

    class Sums:
        def __init__(self, role):
            self.r = role

        def copies(self, stage):
            r = self.r
            if stage == 0:
                return [remote(sbuf.at[r, 0], srecv.at[r, 0], ss_s.at[r, 0], ss_r.at[r, 0], partner)]
            dev = xdev if stage == 1 else ydev
            base = 1 if stage == 1 else RING
            return [remote(sbuf.at[r, stage], srecv.at[r, base + o - 1], ss_s.at[r, base + o - 1],
                           ss_r.at[r, base + o - 1], dev(o)) for o in range(1, RING)]

        def start(self, value):
            sbuf[self.r, 0] = value
            for cp in self.copies(0):
                cp.start()

        def step(self, stage):
            r = self.r
            cps = self.copies(stage - 1)
            total = sbuf[r, stage - 1]
            base = (0, 1, RING)[stage - 1]
            for i, cp in enumerate(cps):
                cp.wait_recv()
                total = total + srecv[r, base + i]
            for cp in cps:
                cp.wait_send()
            if stage < 3:
                sbuf[r, stage] = total
                for cp in self.copies(stage):
                    cp.start()
            else:
                sfin[r] = jnp.broadcast_to(jnp.sum(total, axis=0, keepdims=True), (8, topics))

    wsum, hsum = Sums(0), Sums(1)

    def turn(k):
        for b in range(topics // sh):
            v = hblock(b)[:, hrows(k)].T
            tcols = pl.ds(b * sh, sh)
            hb[0, hrows(k), tcols] = v.astype(BF)

            @pl.when(k == y)
            def _():
                hf[:, tcols] = v
                hb[1, hrows(x), tcols] = v.astype(BF)

    for cp in hloads:
        cp.wait()
    turn(y)
    loads[0].wait()

    @pl.loop(0, sw // EW)
    def _(b):
        rows = pl.ds(mult(b * EW, EW), EW)
        wb[1, pl.ds(mult((y * 2 + c) * sw + b * EW, EW), EW), :] = wf[1, rows, :].astype(BF)

    pl.semaphore_wait(barrier, len(ORDER) + 1)
    for j in range(SUBS):
        hag[1].start(j)
        wag[1].start(j)
    for dx, dy in ORDER:
        c_move(dx, dy).start()
    for o in range(1, RING):
        turn(mod(y + o))
    for b in range(docs // (2 * sw)):
        wload(b).wait()

        @pl.loop(0, 2 * sw // EW)
        def _(e):
            wb[0, pl.ds(mult(b * 2 * sw + e * EW, EW), EW), :] = wacc[b % 2, pl.ds(mult(e * EW, EW), EW), :].astype(BF)
        if b + 2 < docs // (2 * sw):
            wload(b + 2).start()
    for cp in loads[1:]:
        cp.wait()

    def colsum(ref):
        n = ref.shape[0]

        def body(i, tot):
            return tot + ref[pl.ds(mult(i * 8, 8), 8), :]

        return lax.fori_loop(0, n // 8, body, jnp.zeros((8, topics), F32), unroll=4)

    def w_unit(g, s, kk, width, first, halves=(0, 1)):
        p = wpos[g]
        rows = (wrows(mod(p - (1 + s) * d), c), wrows(mod(p + (1 + s) * d), 1 - c))
        rows = [rows[h] for h in halves]
        dst = pl.ds(halves[0] * sw, len(halves) * sw)
        cols = pl.ds(mult(kk * width, width), width)
        hk = hb[g, cols, :]
        wx = jnp.concatenate([wb[g, r, :] for r in rows], axis=0)
        cx = jnp.concatenate([cv[g, r, cols] for r in rows], axis=0)
        z = lax.dot_general(wx, hk, CONTRACT_LAST, preferred_element_type=F32)
        q = (cx.astype(F32) / (z + EPS)).astype(BF)
        a = jnp.dot(q, hk, preferred_element_type=F32)
        if first:
            wacc[g, dst, :] = a
        else:
            wacc[g, dst, :] += a

    def h_part(g, docs0, words_k, acc, first):
        rows = pl.ds(mult(docs0, BLK), BLK)
        cols = hrows(words_k)
        z = lax.dot_general(wb[g, rows, :], hb[g, cols, :], CONTRACT_LAST, preferred_element_type=F32)
        q = (cv[g, rows, cols].astype(F32) / (z + EPS)).astype(BF)
        a = lax.dot_general(q, wb[g, rows, :], CONTRACT_FIRST, preferred_element_type=F32)
        if first:
            acc[g] = a
        else:
            acc[g] += a

    def ring_out(g, ring, stage, s, i, rows_n, s_sem, r_sem, dev, from_stage):
        n = rows_n // SUBS
        rows = pl.ds(i * n, n)
        src = stage.at[g, rows] if from_stage else ring.at[g, s - 1, rows]
        return remote(src, ring.at[g, s, rows], s_sem.at[g, s, i], r_sem.at[g, s, i], dev)

    def w_ring(g, s, i, from_stage):
        return ring_out(g, wring, wst, s, i, sw, wr_s, wr_r, wdev[g](d), from_stage)

    def h_ring(g, s, i, from_stage):
        return ring_out(g, hring, hst, s, i, sh, hr_s, hr_r, hdev[g](d), from_stage)

    def d2d_copy(g, s):
        slot = lax.rem(s, 2)
        return remote(wacc.at[g, pl.ds(sw, sw)], d2d.at[g, slot], d2_s.at[g, slot], d2_r.at[g, slot], partner)

    def w_sweep(t):
        n = sw // SUBS
        orders = [(p, mod(p - d), mod(p + d), mod(p + 2)) for p in hpos]

        @pl.when(t == 0)
        def _():
            got_near([hag[1], wag[1]])
            got_far([hag[1], wag[1]])
            for i in range(4):
                wag[1].got_pair(i)
            hag[1].sent()
            wag[1].sent()
            for dx, dy in ORDER:
                c_in(dx, dy).wait_recv()
                c_move(dx, dy).wait_send()

        for g in range(2):
            w_unit(g, 0, orders[g][0], sh, True)

        @pl.when(t > 0)
        def _():
            got_near(hag)

        hsum.step(1)
        for i in (1, 2):
            for g in range(2):
                w_unit(g, 0, orders[g][i], sh, False)
        hsum.step(2)

        @pl.when(t > 0)
        def _():
            got_far(hag)

        for g in range(2):
            w_unit(g, 0, orders[g][3], sh, False, (1,))
            d2d_copy(g, 0).start()
        for g in range(2):
            w_unit(g, 0, orders[g][3], sh, False, (0,))
        for g in range(2):
            d2d_copy(g, 0).wait_recv()
        for i in range(SUBS):
            for g in range(2):
                @pl.loop(0, n // EW)
                def _(b):
                    rows = pl.ds(mult(i * n + b * EW, EW), EW)
                    wst[g, rows, :] = wacc[g, rows, :] + d2d[g, 0, rows, :]
                w_ring(g, 0, i, True).start()

        @pl.when(t > 0)
        def _():
            for g in range(2):
                hag[g].sent()

        hsum.step(3)
        for g in range(2):
            d2d_copy(g, 0).wait_send()

        @pl.loop(1, RING)
        def _(s):
            for g in range(2):
                w_unit(g, s, 0, words, True)
                d2d_copy(g, s).start()
            slot = lax.rem(s, 2)
            for g in range(2):
                d2d_copy(g, s).wait_recv()

            @pl.when(s < RING - 1)
            def _():
                for i in range(SUBS):
                    for g in range(2):
                        w_ring(g, s - 1, i, True).wait_recv()

                        @pl.loop(0, n // EW)
                        def _(b):
                            rows = pl.ds(mult(i * n + b * EW, EW), EW)
                            wring[g, s - 1, rows, :] = wring[g, s - 1, rows, :] + (wacc[g, rows, :] + d2d[g, slot, rows, :])
                        w_ring(g, s, i, False).start()
            for g in range(2):
                d2d_copy(g, s).wait_send()

        s = RING - 1
        tot = jnp.zeros((8, topics), F32)
        for i in range(SUBS):
            for g in range(2):
                own = (wpos[g] * 2 + c) * sw
                w_ring(g, s - 1, i, False).wait_recv()

                def body(b, tot):
                    r0 = mult(i * n + b * 16, 16)
                    rows = pl.ds(r0, 16)
                    a = wring[g, s - 1, rows, :] + (wacc[g, rows, :] + d2d[g, s % 2, rows, :])
                    new = wf[g, rows, :] * a / jnp.concatenate([sfin[1], sfin[1]], axis=0)
                    wf[g, rows, :] = new
                    wb[g, pl.ds(mult(own + r0, 16), 16), :] = new.astype(BF)
                    return tot + (new[:8] + new[8:])
                tot = lax.fori_loop(0, n // 16, body, tot)
                wag[g].start(i)
        wsum.start(tot)
        for g in range(2):
            for ss in range(RING - 1):
                for i in range(SUBS):
                    w_ring(g, ss, i, ss == 0).wait_send()

    def h_sweep(t):
        n = sh // SUBS
        k0 = [mod(p - d) for p in hpos]

        def chunk(g, delta, first):
            h_part(g, mod(wpos[g] + delta) * BLK, k0[g], hst, first)

        for g in range(2):
            wag[g].got_pair(0)
            chunk(g, 0, True)
        wsum.step(1)
        got_near(wag)
        for g in range(2):
            wag[g].got_pair(2)
            chunk(g, -d, False)
        for g in range(2):
            wag[g].got_pair(1)
            chunk(g, d, False)
        wsum.step(2)
        got_far(wag)
        for g in range(2):
            wag[g].got_pair(3)
            chunk(g, 2, False)
            for i in range(SUBS):
                h_ring(g, 0, i, True).start()
        for g in range(2):
            wag[g].sent()
        wsum.step(3)

        @pl.loop(1, RING)
        def _(s):
            for g in range(2):
                k = mod(hpos[g] - (1 + s) * d)
                h_part(g, 0, k, hacc, True)

                @pl.loop(1, docs // BLK)
                def _(b):
                    h_part(g, b * BLK, k, hacc, False)

            @pl.when(s < RING - 1)
            def _():
                for i in range(SUBS):
                    for g in range(2):
                        h_ring(g, s - 1, i, True).wait_recv()

                        @pl.loop(0, n // EW)
                        def _(b):
                            rows = pl.ds(mult(i * n + b * EW, EW), EW)
                            hring[g, s - 1, rows, :] = hring[g, s - 1, rows, :] + hacc[g, rows, :]
                        h_ring(g, s, i, False).start()

        @pl.when(t == SWEEPS - 1)
        def _():
            for g in range(2):
                for j in range(SUBS):
                    wfin[g].start(j)
                wlocal(g).start()

        s = RING - 1
        tot = jnp.zeros((8, topics), F32)
        for i in range(SUBS):
            for g in range(2):
                h_ring(g, s - 1, i, False).wait_recv()

            def body(b, tot):
                r0 = mult(i * n + b * 16, 16)
                rows = pl.ds(r0, 16)
                a = (hring[0, s - 1, rows, :] + hacc[0, rows, :]) + (hring[1, s - 1, rows, :] + hacc[1, rows, :])
                new = hf[rows, :] * a / jnp.concatenate([sfin[0], sfin[0]], axis=0)
                hf[rows, :] = new
                for g in range(2):
                    hb[g, pl.ds(mult(hpos[g] * sh + r0, 16), 16), :] = new.astype(BF)
                return tot + (new[:8] + new[8:])
            tot = lax.fori_loop(0, n // 16, body, tot)

            @pl.when(t < SWEEPS - 1)
            def _():
                for g in range(2):
                    hag[g].start(i)

            @pl.when(t == SWEEPS - 1)
            def _():
                hfin.start(i)

        @pl.when(t < SWEEPS - 1)
        def _():
            hsum.start(tot)

        for g in range(2):
            for ss in range(RING - 1):
                for i in range(SUBS):
                    h_ring(g, ss, i, ss == 0).wait_send()

    def wlocal(g):
        return pltpu.make_async_copy(wf.at[g], w_out.at[wrows(x, c, g * docs)], ld_sem.at[g])

    hsum.start(colsum(hf))

    @pl.loop(0, SWEEPS)
    def _(t):
        w_sweep(t)
        h_sweep(t)

    hlocal = pltpu.make_async_copy(hf, h_out.at[hrows(y)], ld_sem.at[2])
    hlocal.start()
    got_near([hfin])
    got_near(wfin)
    got_far([hfin])
    got_far(wfin)
    for g in range(2):
        for i in range(4):
            wfin[g].got_pair(i)
        wfin[g].sent()
        wlocal(g).wait()
    hfin.sent()
    hlocal.wait()


def local(c_blk, w_loc, h_loc):
    docs, words = c_blk.shape
    topics = w_loc.shape[1]
    half = docs // 2
    sw, sh = half // (2 * RING), words // RING
    dma = pltpu.SemaphoreType.DMA
    w_out, h_out = pl.pallas_call(
        kernel,
        out_shape=(jax.ShapeDtypeStruct((docs, topics), F32), jax.ShapeDtypeStruct((words, topics), F32)),
        in_specs=[pl.BlockSpec(memory_space=pl.ANY)] * 3,
        out_specs=(pl.BlockSpec(memory_space=pl.ANY), pl.BlockSpec(memory_space=pl.ANY)),
        scratch_shapes=[
            pltpu.VMEM((2, half, words), BF),
            pltpu.VMEM((2, half, topics), BF),
            pltpu.VMEM((2, words, topics), BF),
            pltpu.VMEM((2, sw, topics), F32),
            pltpu.VMEM((sh, topics), F32),
            pltpu.VMEM((2, 2 * sw, topics), F32),
            pltpu.VMEM((2, sh, topics), F32),
            pltpu.VMEM((2, RING - 1, sw, topics), F32),
            pltpu.VMEM((2, RING - 1, sh, topics), F32),
            pltpu.VMEM((2, sw, topics), F32),
            pltpu.VMEM((2, sh, topics), F32),
            pltpu.VMEM((2, 2, sw, topics), F32),
            pltpu.VMEM((2, 3, 8, topics), F32),
            pltpu.VMEM((2, 2 * RING - 1, 8, topics), F32),
            pltpu.VMEM((2, 8, topics), F32),
            dma((13,)),
            dma((RING, RING)), dma((RING, RING)),
            dma((2, RING - 1, SUBS)), dma((2, RING - 1, SUBS)),
            dma((2, RING - 1, SUBS)), dma((2, RING - 1, SUBS)),
            dma((2, 2)), dma((2, 2)),
            dma((7, 3, SUBS)), dma((7, 3, SUBS)),
            dma((7, 4, SUBS)), dma((7, 4, SUBS)),
            dma((2, 2 * RING - 1)), dma((2, 2 * RING - 1)),
        ],
        compiler_params=pltpu.CompilerParams(collective_id=0, has_side_effects=True,
                                             vmem_limit_bytes=63 * 1024 * 1024),
    )(c_blk, w_loc, h_loc)
    return w_out, h_out.T


def solution(mesh):
    spec_c = P(('part', 'row'), 'col')
    spec_w = P(('part', 'row'), None)
    spec_h = P(None, ('part', 'col'))
    return jax.shard_map(local, mesh=mesh, in_specs=(spec_c, spec_w, spec_h), out_specs=(spec_w, spec_h), check_vma=False)
```

```python
import functools

import jax
import jax.numpy as jnp
from jax import lax
from jax.experimental import pallas as pl
from jax.experimental.pallas import tpu as pltpu
from jax.sharding import PartitionSpec as P

SWEEPS = 4
EPS = 1e-6
RING = 4
SUBS = 2
BLK = 512
EW = 32
C_FIRST = ((0, 1), (0, 3), (1, 1), (3, 3), (1, 3), (3, 1), (2, 1), (2, 3))
C_NEXT = ((1, 2), (3, 2), (0, 2), (2, 2))
C_LAST = ((1, 0), (3, 0), (2, 0))
ORDER = C_FIRST + C_NEXT + C_LAST
MESH = pl.DeviceIdType.MESH
F32 = jnp.float32
BF = jnp.bfloat16
CONTRACT_LAST = (((1,), (1,)), ((), ()))
CONTRACT_FIRST = (((0,), (0,)), ((), ()))


def mult(v, m):
    return pl.multiple_of(v, m)


def kernel(c_hbm, w0_hbm, h0_hbm, w_out, h_out,
           cv, wb, hb, wf, hf, wacc, hacc, wring, hring, wst, hst, d2d, sbuf, srecv, sfin,
           ld_sem, c_s, c_r, wr_s, wr_r, hr_s, hr_r, d2_s, d2_r, ag_s, ag_r, pg_s, pg_r, ss_s, ss_r):
    col = lax.axis_index("col")
    y = lax.axis_index("row")
    x, c = col // 2, lax.rem(col, 2)
    d = 1 - 2 * c
    _, docs, topics = wb.shape
    words = hb.shape[1]
    sw = docs // (2 * RING)
    sh = words // RING

    def mod(v):
        return lax.rem(v + 4 * RING, RING)

    def xdev(delta):
        return {"col": mod(x + delta) * 2 + c}

    def ydev(delta):
        return {"row": mod(y + delta)}

    def xydev(dx, dy):
        return {"row": mod(y + dy), "col": mod(x + dx) * 2 + c}

    partner = {"col": x * 2 + (1 - c)}
    wpos, hpos = (x, y), (y, x)
    wdev, hdev = (xdev, ydev), (ydev, xdev)

    def remote(src, dst, s_sem, r_sem, dev):
        return pltpu.make_async_remote_copy(src_ref=src, dst_ref=dst, send_sem=s_sem, recv_sem=r_sem,
                                            device_id=dev, device_id_type=MESH)

    barrier = pltpu.get_barrier_semaphore()
    for dx, dy in ORDER:
        pl.semaphore_signal(barrier, inc=1, device_id=xydev(dx, dy), device_id_type=MESH)
    pl.semaphore_signal(barrier, inc=1, device_id=partner, device_id_type=MESH)

    def wrows(k, h, base=0):
        return pl.ds(mult((k * 2 + h) * sw + base, sw), sw)

    def hrows(k):
        return pl.ds(mult(k * sh, sh), sh)

    def crows(k, base=0):
        return pl.ds(mult(k * 2 * sw + base, 2 * sw), 2 * sw)

    def hblock(b):
        return hring.at[b // (RING - 1), b % (RING - 1)]

    def wload(b):
        return pltpu.make_async_copy(w0_hbm.at[crows(b)], wacc.at[b % 2], ld_sem.at[9 + b])

    loads = [
        pltpu.make_async_copy(w0_hbm.at[wrows(x, c, docs)], wf.at[1], ld_sem.at[0]),
        pltpu.make_async_copy(w0_hbm.at[wrows(x, c)], wf.at[0], ld_sem.at[1]),
        pltpu.make_async_copy(c_hbm.at[pl.ds(0, docs)], cv.at[0], ld_sem.at[2]),
        pltpu.make_async_copy(c_hbm.at[crows(x, docs), hrows(y)], cv.at[1, crows(y), hrows(x)], ld_sem.at[3]),
    ]
    hloads = [pltpu.make_async_copy(h0_hbm.at[hrows(b)], hblock(b), ld_sem.at[4 + b]) for b in range(topics // sh)]
    for cp in hloads + loads + [wload(0), wload(1)]:
        cp.start()

    def c_move(dx, dy):
        return remote(c_hbm.at[crows(mod(x + dx), docs), hrows(mod(y + dy))], cv.at[1, crows(y), hrows(x)],
                      c_s.at[dx, dy], c_r.at[dx, dy], xydev(dx, dy))

    def c_in(dx, dy):
        dst = cv.at[1, crows(mod(y - dy)), hrows(mod(x - dx))]
        return remote(dst, dst, c_s.at[dx, dy], c_r.at[dx, dy], xydev(dx, dy))

    def piece(rows, j):
        n = rows.size // SUBS
        return pl.ds(mult(rows.start + j * n, n), n)

    class Gather:
        def __init__(self, buf, own, slot, pos, dev, rows, is_w):
            self.buf, self.own, self.slot, self.is_w = buf, own, slot, is_w
            self.p, self.dev, self.rows = pos, dev, rows

        def make(self, k, h, j, own, s_sem, r_sem, i, dev):
            rows = self.rows(k, h)
            dst = self.buf.at[piece(rows, j)]
            src = dst
            if own and self.own is not None:
                n = rows.size // SUBS
                src = self.own.at[pl.ds(j * n, n)]
            return remote(src, dst, s_sem.at[self.slot, i, j], r_sem.at[self.slot, i, j], dev)

        def ring(self, i, j):
            k = self.p if i < 2 else mod(self.p - d)
            return self.make(k, c, j, i < 2, ag_s, ag_r, i, self.dev(-d if i == 1 else d))

        def ring_in(self, i, j):
            k = mod(self.p + (-d, d, -2 * d)[i])
            return self.make(k, c, j, False, ag_s, ag_r, i, self.dev(d))

        def pair(self, i, j):
            k = mod(self.p + (0, -d, d, 2)[i])
            return self.make(k, c, j, i == 0, pg_s, pg_r, i, partner)

        def pair_in(self, i, j):
            k = mod(self.p + (0, d, -d, 2)[i])
            return self.make(k, 1 - c, j, False, pg_s, pg_r, i, partner)

        def start(self, j):
            self.ring(0, j).start()
            self.ring(1, j).start()
            if self.is_w:
                self.pair(0, j).start()

        def got(self, i, j):
            self.ring_in(i, j).wait_recv()
            if i == 0:
                self.ring(2, j).start()
            if self.is_w:
                self.pair(i + 1, j).start()

        def got_pair(self, i):
            if self.is_w:
                for j in range(SUBS):
                    self.pair_in(i, j).wait_recv()

        def sent(self):
            for j in range(SUBS):
                for i in range(3):
                    self.ring(i, j).wait_send()
                if self.is_w:
                    for i in range(4):
                        self.pair(i, j).wait_send()

    def got_near(gathers):
        for j in range(SUBS):
            for i in range(2):
                for ga in gathers:
                    ga.got(i, j)

    def got_far(gathers):
        for j in range(SUBS):
            for ga in gathers:
                ga.got(2, j)

    wag = [Gather(wb.at[g], None, g, wpos[g], wdev[g], wrows, True) for g in range(2)]
    hag = [Gather(hb.at[g], None, 2 + g, hpos[g], hdev[g], lambda k, h: hrows(k), False) for g in range(2)]
    wfin = [Gather(w_out, wf.at[g], 4 + g, x, xdev, functools.partial(wrows, base=g * docs), True) for g in range(2)]
    hfin = Gather(h_out, hf, 6, y, ydev, lambda k, h: hrows(k), False)

    class Sums:
        def __init__(self, role):
            self.r = role

        def copies(self, stage):
            r = self.r
            if stage == 0:
                return [remote(sbuf.at[r, 0], srecv.at[r, 0], ss_s.at[r, 0], ss_r.at[r, 0], partner)]
            dev = xdev if stage == 1 else ydev
            base = 1 if stage == 1 else RING
            return [remote(sbuf.at[r, stage], srecv.at[r, base + o - 1], ss_s.at[r, base + o - 1],
                           ss_r.at[r, base + o - 1], dev(o)) for o in range(1, RING)]

        def start(self, value):
            sbuf[self.r, 0] = value
            for cp in self.copies(0):
                cp.start()

        def step(self, stage):
            r = self.r
            cps = self.copies(stage - 1)
            total = sbuf[r, stage - 1]
            base = (0, 1, RING)[stage - 1]
            for i, cp in enumerate(cps):
                cp.wait_recv()
                total = total + srecv[r, base + i]
            for cp in cps:
                cp.wait_send()
            if stage < 3:
                sbuf[r, stage] = total
                for cp in self.copies(stage):
                    cp.start()
            else:
                sfin[r] = jnp.broadcast_to(jnp.sum(total, axis=0, keepdims=True), (8, topics))

    wsum, hsum = Sums(0), Sums(1)

    def turn(k):
        for b in range(topics // sh):
            v = hblock(b)[:, hrows(k)].T
            tcols = pl.ds(b * sh, sh)
            hb[0, hrows(k), tcols] = v.astype(BF)

            @pl.when(k == y)
            def _():
                hf[:, tcols] = v
                hb[1, hrows(x), tcols] = v.astype(BF)

    pl.semaphore_wait(barrier, len(ORDER) + 1)
    for dx, dy in ORDER[:8]:
        c_move(dx, dy).start()
    for cp in hloads:
        cp.wait()
    turn(y)
    loads[0].wait()

    @pl.loop(0, sw // EW)
    def _(b):
        rows = pl.ds(mult(b * EW, EW), EW)
        wb[1, pl.ds(mult((y * 2 + c) * sw + b * EW, EW), EW), :] = wf[1, rows, :].astype(BF)

    for j in range(SUBS):
        hag[1].start(j)
        wag[1].start(j)
    for dx, dy in ORDER[8:]:
        c_move(dx, dy).start()
    for o in range(1, RING):
        turn(mod(y + o))
    for b in range(docs // (2 * sw)):
        wload(b).wait()

        @pl.loop(0, 2 * sw // EW)
        def _(e):
            wb[0, pl.ds(mult(b * 2 * sw + e * EW, EW), EW), :] = wacc[b % 2, pl.ds(mult(e * EW, EW), EW), :].astype(BF)
        if b + 2 < docs // (2 * sw):
            wload(b + 2).start()
    for cp in loads[1:]:
        cp.wait()

    def colsum(ref):
        n = ref.shape[0]

        def body(i, tot):
            return tot + ref[pl.ds(mult(i * 8, 8), 8), :]

        return lax.fori_loop(0, n // 8, body, jnp.zeros((8, topics), F32), unroll=4)

    def w_unit(g, s, kk, width, first, halves=(0, 1)):
        p = wpos[g]
        rows = (wrows(mod(p - (1 + s) * d), c), wrows(mod(p + (1 + s) * d), 1 - c))
        rows = [rows[h] for h in halves]
        dst = pl.ds(halves[0] * sw, len(halves) * sw)
        cols = pl.ds(mult(kk * width, width), width)
        hk = hb[g, cols, :]
        wx = jnp.concatenate([wb[g, r, :] for r in rows], axis=0)
        cx = jnp.concatenate([cv[g, r, cols] for r in rows], axis=0)
        z = lax.dot_general(wx, hk, CONTRACT_LAST, preferred_element_type=F32)
        q = (cx.astype(F32) / (z + EPS)).astype(BF)
        a = jnp.dot(q, hk, preferred_element_type=F32)
        if first:
            wacc[g, dst, :] = a
        else:
            wacc[g, dst, :] += a

    def h_part(g, docs0, words_k, acc, first, blk=BLK):
        rows = pl.ds(mult(docs0, blk), blk)
        cols = hrows(words_k)
        z = lax.dot_general(wb[g, rows, :], hb[g, cols, :], CONTRACT_LAST, preferred_element_type=F32)
        q = (cv[g, rows, cols].astype(F32) / (z + EPS)).astype(BF)
        a = lax.dot_general(q, wb[g, rows, :], CONTRACT_FIRST, preferred_element_type=F32)
        if first:
            acc[g] = a
        else:
            acc[g] += a

    def ring_out(g, ring, stage, s, i, rows_n, s_sem, r_sem, dev, from_stage):
        n = rows_n // SUBS
        rows = pl.ds(i * n, n)
        src = stage.at[g, rows] if from_stage else ring.at[g, s - 1, rows]
        return remote(src, ring.at[g, s, rows], s_sem.at[g, s, i], r_sem.at[g, s, i], dev)

    def w_ring(g, s, i, from_stage):
        return ring_out(g, wring, wst, s, i, sw, wr_s, wr_r, wdev[g](d), from_stage)

    def h_ring(g, s, i, from_stage):
        return ring_out(g, hring, hst, s, i, sh, hr_s, hr_r, hdev[g](d), from_stage)

    def d2d_copy(g, s, i):
        slot = lax.rem(s, 2)
        n = sw // SUBS
        return remote(wacc.at[g, pl.ds(sw + i * n, n)], d2d.at[g, slot, pl.ds(i * n, n)],
                      d2_s.at[g, slot, i], d2_r.at[g, slot, i], partner)

    def w_sweep(t):
        n = sw // SUBS
        orders = [(p, mod(p - d), mod(p + d), mod(p + 2)) for p in hpos]

        w_unit(0, 0, orders[0][0], sh, True)

        @pl.when(t == 0)
        def _():
            got_near([hag[1], wag[1]])
            got_far([hag[1], wag[1]])
            for i in range(4):
                wag[1].got_pair(i)
            hag[1].sent()
            wag[1].sent()
            for dx, dy in C_FIRST:
                c_in(dx, dy).wait_recv()

        w_unit(1, 0, orders[1][0], sh, True)

        @pl.when(t > 0)
        def _():
            got_near(hag)

        hsum.step(1)
        for i in (1, 2):
            for g in range(2):
                w_unit(g, 0, orders[g][i], sh, False)
        hsum.step(2)

        @pl.when(t > 0)
        def _():
            got_far(hag)

        for g in range(2):
            w_unit(g, 0, orders[g][3], sh, False, (1,))
            for i in range(SUBS):
                d2d_copy(g, 0, i).start()
        for g in range(2):
            w_unit(g, 0, orders[g][3], sh, False, (0,))
        for i in range(SUBS):
            for g in range(2):
                d2d_copy(g, 0, i).wait_recv()

                @pl.loop(0, n // EW)
                def _(b):
                    rows = pl.ds(mult(i * n + b * EW, EW), EW)
                    wst[g, rows, :] = wacc[g, rows, :] + d2d[g, 0, rows, :]
                w_ring(g, 0, i, True).start()

        @pl.when(t > 0)
        def _():
            for g in range(2):
                hag[g].sent()

        hsum.step(3)
        for g in range(2):
            for i in range(SUBS):
                d2d_copy(g, 0, i).wait_send()

        @pl.loop(1, RING)
        def _(s):
            for g in range(2):
                if g == 1:
                    @pl.when(jnp.logical_and(t == 0, s == 1))
                    def _():
                        for dx, dy in C_NEXT:
                            c_in(dx, dy).wait_recv()

                    @pl.when(jnp.logical_and(t == 0, s == RING - 1))
                    def _():
                        for dx, dy in C_LAST:
                            c_in(dx, dy).wait_recv()
                        for dx, dy in ORDER:
                            c_move(dx, dy).wait_send()
                w_unit(g, s, 0, words, True)
                for i in range(SUBS):
                    d2d_copy(g, s, i).start()
            slot = lax.rem(s, 2)
            for g in range(2):
                for i in range(SUBS):
                    d2d_copy(g, s, i).wait_recv()

            @pl.when(s < RING - 1)
            def _():
                for i in range(SUBS):
                    for g in range(2):
                        w_ring(g, s - 1, i, True).wait_recv()

                        @pl.loop(0, n // EW)
                        def _(b):
                            rows = pl.ds(mult(i * n + b * EW, EW), EW)
                            wring[g, s - 1, rows, :] = wring[g, s - 1, rows, :] + (wacc[g, rows, :] + d2d[g, slot, rows, :])
                        w_ring(g, s, i, False).start()
            for g in range(2):
                for i in range(SUBS):
                    d2d_copy(g, s, i).wait_send()

        s = RING - 1
        tot = jnp.zeros((8, topics), F32)
        for i in range(SUBS):
            for g in range(2):
                own = (wpos[g] * 2 + c) * sw
                w_ring(g, s - 1, i, False).wait_recv()

                def body(b, tot):
                    r0 = mult(i * n + b * 16, 16)
                    rows = pl.ds(r0, 16)
                    a = wring[g, s - 1, rows, :] + (wacc[g, rows, :] + d2d[g, s % 2, rows, :])
                    new = wf[g, rows, :] * a / jnp.concatenate([sfin[1], sfin[1]], axis=0)
                    wf[g, rows, :] = new
                    wb[g, pl.ds(mult(own + r0, 16), 16), :] = new.astype(BF)
                    return tot + (new[:8] + new[8:])
                tot = lax.fori_loop(0, n // 16, body, tot)
                if g == 0:
                    @pl.when(t < SWEEPS - 1)
                    def _():
                        wag[0].start(i)

                    @pl.when(t == SWEEPS - 1)
                    def _():
                        wfin[0].start(i)
                else:
                    wag[1].start(i)
        wsum.start(tot)
        for g in range(2):
            for ss in range(RING - 1):
                for i in range(SUBS):
                    w_ring(g, ss, i, ss == 0).wait_send()

    def h_sweep(t):
        n = sh // SUBS
        k0 = [mod(p - d) for p in hpos]

        def chunk(g, delta, first):
            h_part(g, mod(wpos[g] + delta) * BLK, k0[g], hst, first)

        last = t == SWEEPS - 1

        def fetch(delta, halves):
            k = mod(x + delta)
            cps = [pltpu.make_async_copy(w_out.at[wrows(k, h)], wring.at[0, i], ld_sem.at[2 + i])
                   for i, h in enumerate(halves)]
            for cp in cps:
                cp.start()
            for i, h in enumerate(halves):
                cps[i].wait()

                @pl.loop(0, sw // EW)
                def _(e):
                    rows = pl.ds(mult((k * 2 + h) * sw + e * EW, EW), EW)
                    wb[0, rows, :] = wring[0, i, pl.ds(mult(e * EW, EW), EW), :].astype(BF)

        def have(i, delta, halves):
            @pl.when(jnp.logical_not(last))
            def _():
                wag[0].got_pair(i)

            @pl.when(last)
            def _():
                wfin[0].got_pair(i)
                fetch(delta, halves)

        have(0, 0, (1 - c,))
        wag[1].got_pair(0)
        for g in range(2):
            chunk(g, 0, True)
        wsum.step(1)

        @pl.when(jnp.logical_not(last))
        def _():
            got_near(wag)

        @pl.when(last)
        def _():
            got_near([wfin[0], wag[1]])

        for i, delta in ((2, -d), (1, d)):
            have(i, delta, (0, 1))
            wag[1].got_pair(i)
            for g in range(2):
                chunk(g, delta, False)
        wsum.step(2)

        @pl.when(jnp.logical_not(last))
        def _():
            got_far(wag)

        @pl.when(last)
        def _():
            got_far([wfin[0], wag[1]])

        @pl.when(last)
        def _():
            fetch(2, (c,))

        def far_half(g, h):
            h_part(g, (mod(wpos[g] + 2) * 2 + h) * sw, k0[g], hst, False, sw)

        for g in range(2):
            far_half(g, c)
        have(3, 2, (1 - c,))
        wag[1].got_pair(3)
        for g in range(2):
            far_half(g, 1 - c)
            for i in range(SUBS):
                h_ring(g, 0, i, True).start()
        wag[1].sent()

        @pl.when(jnp.logical_not(last))
        def _():
            wag[0].sent()

        wsum.step(3)

        @pl.loop(1, RING)
        def _(s):
            for g in range(2):
                k = mod(hpos[g] - (1 + s) * d)
                h_part(g, 0, k, hacc, True)

                @pl.loop(1, docs // BLK)
                def _(b):
                    h_part(g, b * BLK, k, hacc, False)

            @pl.when(s < RING - 1)
            def _():
                for i in range(SUBS):
                    for g in range(2):
                        h_ring(g, s - 1, i, True).wait_recv()

                        @pl.loop(0, n // EW)
                        def _(b):
                            rows = pl.ds(mult(i * n + b * EW, EW), EW)
                            hring[g, s - 1, rows, :] = hring[g, s - 1, rows, :] + hacc[g, rows, :]
                        h_ring(g, s, i, False).start()

        @pl.when(t == SWEEPS - 1)
        def _():
            for j in range(SUBS):
                wfin[1].start(j)
            for g in range(2):
                wlocal(g).start()

        s = RING - 1
        tot = jnp.zeros((8, topics), F32)
        for i in range(SUBS):
            for g in range(2):
                h_ring(g, s - 1, i, False).wait_recv()

            def body(b, tot):
                r0 = mult(i * n + b * 16, 16)
                rows = pl.ds(r0, 16)
                a = (hring[0, s - 1, rows, :] + hacc[0, rows, :]) + (hring[1, s - 1, rows, :] + hacc[1, rows, :])
                new = hf[rows, :] * a / jnp.concatenate([sfin[0], sfin[0]], axis=0)
                hf[rows, :] = new
                for g in range(2):
                    hb[g, pl.ds(mult(hpos[g] * sh + r0, 16), 16), :] = new.astype(BF)
                return tot + (new[:8] + new[8:])
            tot = lax.fori_loop(0, n // 16, body, tot)

            @pl.when(t < SWEEPS - 1)
            def _():
                for g in range(2):
                    hag[g].start(i)

            @pl.when(t == SWEEPS - 1)
            def _():
                hfin.start(i)

        @pl.when(t < SWEEPS - 1)
        def _():
            hsum.start(tot)

        for g in range(2):
            for ss in range(RING - 1):
                for i in range(SUBS):
                    h_ring(g, ss, i, ss == 0).wait_send()

    def wlocal(g):
        return pltpu.make_async_copy(wf.at[g], w_out.at[wrows(x, c, g * docs)], ld_sem.at[g])

    hsum.start(colsum(hf))

    @pl.loop(0, SWEEPS)
    def _(t):
        w_sweep(t)
        h_sweep(t)

    hlocal = pltpu.make_async_copy(hf, h_out.at[hrows(y)], ld_sem.at[2])
    hlocal.start()
    got_near([wfin[1], hfin])
    got_far([wfin[1], hfin])
    for g in range(2):
        if g == 1:
            for i in range(4):
                wfin[1].got_pair(i)
        wfin[g].sent()
        wlocal(g).wait()
    hfin.sent()
    hlocal.wait()


def local(c_blk, w_loc, h_loc):
    docs, words = c_blk.shape
    topics = w_loc.shape[1]
    half = docs // 2
    sw, sh = half // (2 * RING), words // RING
    dma = pltpu.SemaphoreType.DMA
    w_out, h_out = pl.pallas_call(
        kernel,
        out_shape=(jax.ShapeDtypeStruct((docs, topics), F32), jax.ShapeDtypeStruct((words, topics), F32)),
        in_specs=[pl.BlockSpec(memory_space=pl.ANY)] * 3,
        out_specs=(pl.BlockSpec(memory_space=pl.ANY), pl.BlockSpec(memory_space=pl.ANY)),
        scratch_shapes=[
            pltpu.VMEM((2, half, words), BF),
            pltpu.VMEM((2, half, topics), BF),
            pltpu.VMEM((2, words, topics), BF),
            pltpu.VMEM((2, sw, topics), F32),
            pltpu.VMEM((sh, topics), F32),
            pltpu.VMEM((2, 2 * sw, topics), F32),
            pltpu.VMEM((2, sh, topics), F32),
            pltpu.VMEM((2, RING - 1, sw, topics), F32),
            pltpu.VMEM((2, RING - 1, sh, topics), F32),
            pltpu.VMEM((2, sw, topics), F32),
            pltpu.VMEM((2, sh, topics), F32),
            pltpu.VMEM((2, 2, sw, topics), F32),
            pltpu.VMEM((2, 3, 8, topics), F32),
            pltpu.VMEM((2, 2 * RING - 1, 8, topics), F32),
            pltpu.VMEM((2, 8, topics), F32),
            dma((13,)),
            dma((RING, RING)), dma((RING, RING)),
            dma((2, RING - 1, SUBS)), dma((2, RING - 1, SUBS)),
            dma((2, RING - 1, SUBS)), dma((2, RING - 1, SUBS)),
            dma((2, 2, SUBS)), dma((2, 2, SUBS)),
            dma((7, 3, SUBS)), dma((7, 3, SUBS)),
            dma((7, 4, SUBS)), dma((7, 4, SUBS)),
            dma((2, 2 * RING - 1)), dma((2, 2 * RING - 1)),
        ],
        compiler_params=pltpu.CompilerParams(collective_id=0, has_side_effects=True,
                                             vmem_limit_bytes=63 * 1024 * 1024),
    )(c_blk, w_loc, h_loc)
    return w_out, h_out.T


def solution(mesh):
    spec_c = P(('part', 'row'), 'col')
    spec_w = P(('part', 'row'), None)
    spec_h = P(None, ('part', 'col'))
    return jax.shard_map(local, mesh=mesh, in_specs=(spec_c, spec_w, spec_h), out_specs=(spec_w, spec_h), check_vma=False)
```

```python
import functools

import jax
import jax.numpy as jnp
from jax import lax
from jax.experimental import pallas as pl
from jax.experimental.pallas import tpu as pltpu
from jax.sharding import PartitionSpec as P

SWEEPS = 4
EPS = 1e-6
RING = 4
SUBS = 2
BLK = 512
EW = 32
C_FIRST = ((0, 1), (0, 3), (1, 1), (3, 3), (1, 3), (3, 1), (2, 1), (2, 3))
C_NEXT = ((1, 2), (3, 2), (0, 2), (2, 2))
C_LAST = ((1, 0), (3, 0), (2, 0))
ORDER = C_FIRST + C_NEXT + C_LAST
MESH = pl.DeviceIdType.MESH
F32 = jnp.float32
BF = jnp.bfloat16
CONTRACT_LAST = (((1,), (1,)), ((), ()))
CONTRACT_FIRST = (((0,), (0,)), ((), ()))


def mult(v, m):
    return pl.multiple_of(v, m)


def kernel(c_hbm, w0_hbm, h0_hbm, w_out, h_out,
           cv, wb, hb, wf, hf, wacc, hacc, wring, hring, wst, hst, d2d, sbuf, srecv, sfin,
           ld_sem, c_s, c_r, wr_s, wr_r, hr_s, hr_r, d2_s, d2_r, ag_s, ag_r, pg_s, pg_r, ss_s, ss_r):
    col = lax.axis_index("col")
    y = lax.axis_index("row")
    x, c = col // 2, lax.rem(col, 2)
    d = 1 - 2 * c
    _, docs, topics = wb.shape
    words = hb.shape[1]
    sw = docs // (2 * RING)
    sh = words // RING

    def mod(v):
        return lax.rem(v + 4 * RING, RING)

    def xdev(delta):
        return {"col": mod(x + delta) * 2 + c}

    def ydev(delta):
        return {"row": mod(y + delta)}

    def xydev(dx, dy):
        return {"row": mod(y + dy), "col": mod(x + dx) * 2 + c}

    partner = {"col": x * 2 + (1 - c)}
    wpos, hpos = (x, y), (y, x)
    wdev, hdev = (xdev, ydev), (ydev, xdev)

    def remote(src, dst, s_sem, r_sem, dev):
        return pltpu.make_async_remote_copy(src_ref=src, dst_ref=dst, send_sem=s_sem, recv_sem=r_sem,
                                            device_id=dev, device_id_type=MESH)

    barrier = pltpu.get_barrier_semaphore()
    for dx, dy in ORDER:
        pl.semaphore_signal(barrier, inc=1, device_id=xydev(dx, dy), device_id_type=MESH)
    pl.semaphore_signal(barrier, inc=1, device_id=partner, device_id_type=MESH)

    def wrows(k, h, base=0):
        return pl.ds(mult((k * 2 + h) * sw + base, sw), sw)

    def hrows(k):
        return pl.ds(mult(k * sh, sh), sh)

    def crows(k, base=0):
        return pl.ds(mult(k * 2 * sw + base, 2 * sw), 2 * sw)

    def hblock(b):
        return hring.at[b // (RING - 1), b % (RING - 1)]

    def wload(b):
        return pltpu.make_async_copy(w0_hbm.at[crows(b)], wacc.at[b % 2], ld_sem.at[9 + b])

    loads = [
        pltpu.make_async_copy(w0_hbm.at[wrows(x, c, docs)], wf.at[1], ld_sem.at[0]),
        pltpu.make_async_copy(w0_hbm.at[wrows(x, c)], wf.at[0], ld_sem.at[1]),
        pltpu.make_async_copy(c_hbm.at[pl.ds(0, docs)], cv.at[0], ld_sem.at[2]),
        pltpu.make_async_copy(c_hbm.at[crows(x, docs), hrows(y)], cv.at[1, crows(y), hrows(x)], ld_sem.at[3]),
    ]
    hloads = [pltpu.make_async_copy(h0_hbm.at[hrows(b)], hblock(b), ld_sem.at[4 + b]) for b in range(topics // sh)]
    for cp in hloads + loads + [wload(0), wload(1)]:
        cp.start()

    def c_move(dx, dy):
        return remote(c_hbm.at[crows(mod(x + dx), docs), hrows(mod(y + dy))], cv.at[1, crows(y), hrows(x)],
                      c_s.at[dx, dy], c_r.at[dx, dy], xydev(dx, dy))

    def c_in(dx, dy):
        dst = cv.at[1, crows(mod(y - dy)), hrows(mod(x - dx))]
        return remote(dst, dst, c_s.at[dx, dy], c_r.at[dx, dy], xydev(dx, dy))

    def piece(rows, j):
        n = rows.size // SUBS
        return pl.ds(mult(rows.start + j * n, n), n)

    class Gather:
        def __init__(self, buf, own, slot, pos, dev, rows, is_w):
            self.buf, self.own, self.slot, self.is_w = buf, own, slot, is_w
            self.p, self.dev, self.rows = pos, dev, rows

        def make(self, k, h, j, own, s_sem, r_sem, i, dev):
            rows = self.rows(k, h)
            dst = self.buf.at[piece(rows, j)]
            src = dst
            if own and self.own is not None:
                n = rows.size // SUBS
                src = self.own.at[pl.ds(j * n, n)]
            return remote(src, dst, s_sem.at[self.slot, i, j], r_sem.at[self.slot, i, j], dev)

        def ring(self, i, j):
            k = self.p if i < 2 else mod(self.p - d)
            return self.make(k, c, j, i < 2, ag_s, ag_r, i, self.dev(-d if i == 1 else d))

        def ring_in(self, i, j):
            k = mod(self.p + (-d, d, -2 * d)[i])
            return self.make(k, c, j, False, ag_s, ag_r, i, self.dev(d))

        def pair(self, i, j):
            k = mod(self.p + (0, -d, d, 2)[i])
            return self.make(k, c, j, i == 0, pg_s, pg_r, i, partner)

        def pair_in(self, i, j):
            k = mod(self.p + (0, d, -d, 2)[i])
            return self.make(k, 1 - c, j, False, pg_s, pg_r, i, partner)

        def start(self, j):
            self.ring(0, j).start()
            self.ring(1, j).start()
            if self.is_w:
                self.pair(0, j).start()

        def got(self, i, j):
            self.ring_in(i, j).wait_recv()
            if i == 0:
                self.ring(2, j).start()
            if self.is_w:
                self.pair(i + 1, j).start()

        def got_pair(self, i):
            if self.is_w:
                for j in range(SUBS):
                    self.pair_in(i, j).wait_recv()

        def sent(self):
            for j in range(SUBS):
                for i in range(3):
                    self.ring(i, j).wait_send()
                if self.is_w:
                    for i in range(4):
                        self.pair(i, j).wait_send()

    def got_near(gathers):
        for j in range(SUBS):
            for i in range(2):
                for ga in gathers:
                    ga.got(i, j)

    def got_far(gathers):
        for j in range(SUBS):
            for ga in gathers:
                ga.got(2, j)

    wag = [Gather(wb.at[g], None, g, wpos[g], wdev[g], wrows, True) for g in range(2)]
    hag = [Gather(hb.at[g], None, 2 + g, hpos[g], hdev[g], lambda k, h: hrows(k), False) for g in range(2)]
    wfin = [Gather(w_out, wf.at[g], 4 + g, x, xdev, functools.partial(wrows, base=g * docs), True) for g in range(2)]
    hfin = Gather(h_out, hf, 6, y, ydev, lambda k, h: hrows(k), False)

    class Sums:
        def __init__(self, role):
            self.r = role

        def copies(self, stage):
            r = self.r
            if stage == 0:
                return [remote(sbuf.at[r, 0], srecv.at[r, 0], ss_s.at[r, 0], ss_r.at[r, 0], partner)]
            dev = xdev if stage == 1 else ydev
            base = 1 if stage == 1 else RING
            return [remote(sbuf.at[r, stage], srecv.at[r, base + o - 1], ss_s.at[r, base + o - 1],
                           ss_r.at[r, base + o - 1], dev(o)) for o in range(1, RING)]

        def start(self, value):
            sbuf[self.r, 0] = value
            for cp in self.copies(0):
                cp.start()

        def step(self, stage):
            r = self.r
            cps = self.copies(stage - 1)
            total = sbuf[r, stage - 1]
            base = (0, 1, RING)[stage - 1]
            for i, cp in enumerate(cps):
                cp.wait_recv()
                total = total + srecv[r, base + i]
            for cp in cps:
                cp.wait_send()
            if stage < 3:
                sbuf[r, stage] = total
                for cp in self.copies(stage):
                    cp.start()
            else:
                sfin[r] = jnp.broadcast_to(jnp.sum(total, axis=0, keepdims=True), (8, topics))

    wsum, hsum = Sums(0), Sums(1)

    def turn(k):
        for b in range(topics // sh):
            v = hblock(b)[:, hrows(k)].T
            tcols = pl.ds(b * sh, sh)
            hb[0, hrows(k), tcols] = v.astype(BF)

            @pl.when(k == y)
            def _():
                hf[:, tcols] = v
                hb[1, hrows(x), tcols] = v.astype(BF)

    pl.semaphore_wait(barrier, len(ORDER) + 1)
    for dx, dy in C_FIRST:
        c_move(dx, dy).start()
    for cp in hloads:
        cp.wait()
    turn(y)
    loads[0].wait()

    @pl.loop(0, sw // EW)
    def _(b):
        rows = pl.ds(mult(b * EW, EW), EW)
        wb[1, pl.ds(mult((y * 2 + c) * sw + b * EW, EW), EW), :] = wf[1, rows, :].astype(BF)

    for j in range(SUBS):
        hag[1].start(j)
        wag[1].start(j)
    for o in range(1, RING):
        turn(mod(y + o))
    for b in range(docs // (2 * sw)):
        wload(b).wait()

        @pl.loop(0, 2 * sw // EW)
        def _(e):
            wb[0, pl.ds(mult(b * 2 * sw + e * EW, EW), EW), :] = wacc[b % 2, pl.ds(mult(e * EW, EW), EW), :].astype(BF)
        if b + 2 < docs // (2 * sw):
            wload(b + 2).start()
    for cp in loads[1:]:
        cp.wait()

    def colsum(ref):
        n = ref.shape[0]

        def body(i, tot):
            return tot + ref[pl.ds(mult(i * 8, 8), 8), :]

        return lax.fori_loop(0, n // 8, body, jnp.zeros((8, topics), F32), unroll=4)

    def w_unit(g, s, kk, width, first, halves=(0, 1)):
        p = wpos[g]
        rows = (wrows(mod(p - (1 + s) * d), c), wrows(mod(p + (1 + s) * d), 1 - c))
        rows = [rows[h] for h in halves]
        dst = pl.ds(halves[0] * sw, len(halves) * sw)
        cols = pl.ds(mult(kk * width, width), width)
        hk = hb[g, cols, :]
        wx = jnp.concatenate([wb[g, r, :] for r in rows], axis=0)
        cx = jnp.concatenate([cv[g, r, cols] for r in rows], axis=0)
        z = lax.dot_general(wx, hk, CONTRACT_LAST, preferred_element_type=F32)
        q = (cx.astype(F32) / (z + EPS)).astype(BF)
        a = jnp.dot(q, hk, preferred_element_type=F32)
        if first:
            wacc[g, dst, :] = a
        else:
            wacc[g, dst, :] += a

    def h_part(g, docs0, words_k, acc, first, blk=BLK):
        rows = pl.ds(mult(docs0, blk), blk)
        cols = hrows(words_k)
        z = lax.dot_general(wb[g, rows, :], hb[g, cols, :], CONTRACT_LAST, preferred_element_type=F32)
        q = (cv[g, rows, cols].astype(F32) / (z + EPS)).astype(BF)
        a = lax.dot_general(q, wb[g, rows, :], CONTRACT_FIRST, preferred_element_type=F32)
        if first:
            acc[g] = a
        else:
            acc[g] += a

    def ring_out(g, ring, stage, s, i, rows_n, s_sem, r_sem, dev, from_stage):
        n = rows_n // SUBS
        rows = pl.ds(i * n, n)
        src = stage.at[g, rows] if from_stage else ring.at[g, s - 1, rows]
        return remote(src, ring.at[g, s, rows], s_sem.at[g, s, i], r_sem.at[g, s, i], dev)

    def w_ring(g, s, i, from_stage):
        return ring_out(g, wring, wst, s, i, sw, wr_s, wr_r, wdev[g](d), from_stage)

    def h_ring(g, s, i, from_stage):
        return ring_out(g, hring, hst, s, i, sh, hr_s, hr_r, hdev[g](d), from_stage)

    def d2d_copy(g, s, i):
        slot = lax.rem(s, 2)
        n = sw // SUBS
        return remote(wacc.at[g, pl.ds(sw + i * n, n)], d2d.at[g, slot, pl.ds(i * n, n)],
                      d2_s.at[g, slot, i], d2_r.at[g, slot, i], partner)

    def w_sweep(t):
        n = sw // SUBS
        orders = [(p, mod(p - d), mod(p + d), mod(p + 2)) for p in hpos]

        w_unit(0, 0, orders[0][0], sh, True)

        @pl.when(t == 0)
        def _():
            got_near([hag[1], wag[1]])
            for dx, dy in C_NEXT + C_LAST:
                c_move(dx, dy).start()
            got_far([hag[1], wag[1]])
            for i in range(4):
                wag[1].got_pair(i)
            hag[1].sent()
            wag[1].sent()
            for dx, dy in C_FIRST:
                c_in(dx, dy).wait_recv()

        w_unit(1, 0, orders[1][0], sh, True)

        @pl.when(t > 0)
        def _():
            got_near(hag)

        hsum.step(1)
        for i in (1, 2):
            for g in range(2):
                w_unit(g, 0, orders[g][i], sh, False)
        @pl.when(t > 0)
        def _():
            got_far(hag)

        for g in range(2):
            w_unit(g, 0, orders[g][3], sh, False, (1,))
            for i in range(SUBS):
                d2d_copy(g, 0, i).start()
        for g in range(2):
            w_unit(g, 0, orders[g][3], sh, False, (0,))
        for i in range(SUBS):
            for g in range(2):
                d2d_copy(g, 0, i).wait_recv()

                @pl.loop(0, n // EW)
                def _(b):
                    rows = pl.ds(mult(i * n + b * EW, EW), EW)
                    wst[g, rows, :] = wacc[g, rows, :] + d2d[g, 0, rows, :]
                w_ring(g, 0, i, True).start()

        @pl.when(t > 0)
        def _():
            for g in range(2):
                hag[g].sent()

        hsum.step(2)
        for g in range(2):
            for i in range(SUBS):
                d2d_copy(g, 0, i).wait_send()

        @pl.loop(1, RING)
        def _(s):
            for g in range(2):
                if g == 1:
                    @pl.when(jnp.logical_and(t == 0, s == 1))
                    def _():
                        for dx, dy in C_NEXT:
                            c_in(dx, dy).wait_recv()

                    @pl.when(jnp.logical_and(t == 0, s == RING - 1))
                    def _():
                        for dx, dy in C_LAST:
                            c_in(dx, dy).wait_recv()
                        for dx, dy in ORDER:
                            c_move(dx, dy).wait_send()
                w_unit(g, s, 0, words, True)
                for i in range(SUBS):
                    d2d_copy(g, s, i).start()
            slot = lax.rem(s, 2)
            for g in range(2):
                for i in range(SUBS):
                    d2d_copy(g, s, i).wait_recv()

            @pl.when(s < RING - 1)
            def _():
                for i in range(SUBS):
                    for g in range(2):
                        w_ring(g, s - 1, i, True).wait_recv()

                        @pl.loop(0, n // EW)
                        def _(b):
                            rows = pl.ds(mult(i * n + b * EW, EW), EW)
                            wring[g, s - 1, rows, :] = wring[g, s - 1, rows, :] + (wacc[g, rows, :] + d2d[g, slot, rows, :])
                        w_ring(g, s, i, False).start()
            for g in range(2):
                for i in range(SUBS):
                    d2d_copy(g, s, i).wait_send()

        hsum.step(3)
        s = RING - 1
        tot = jnp.zeros((8, topics), F32)
        for i in range(SUBS):
            for g in range(2):
                own = (wpos[g] * 2 + c) * sw
                w_ring(g, s - 1, i, False).wait_recv()

                def body(b, tot):
                    r0 = mult(i * n + b * 16, 16)
                    rows = pl.ds(r0, 16)
                    a = wring[g, s - 1, rows, :] + (wacc[g, rows, :] + d2d[g, s % 2, rows, :])
                    new = wf[g, rows, :] * a / jnp.concatenate([sfin[1], sfin[1]], axis=0)
                    wf[g, rows, :] = new
                    wb[g, pl.ds(mult(own + r0, 16), 16), :] = new.astype(BF)
                    return tot + (new[:8] + new[8:])
                tot = lax.fori_loop(0, n // 16, body, tot)
                if g == 0:
                    @pl.when(t < SWEEPS - 1)
                    def _():
                        wag[0].start(i)

                    @pl.when(t == SWEEPS - 1)
                    def _():
                        wfin[0].start(i)
                else:
                    wag[1].start(i)
        wsum.start(tot)
        for g in range(2):
            for ss in range(RING - 1):
                for i in range(SUBS):
                    w_ring(g, ss, i, ss == 0).wait_send()

    def h_sweep(t):
        n = sh // SUBS
        k0 = [mod(p - d) for p in hpos]

        def chunk(g, delta, first):
            h_part(g, mod(wpos[g] + delta) * BLK, k0[g], hst, first)

        last = t == SWEEPS - 1

        def fetch(delta, halves):
            k = mod(x + delta)
            cps = [pltpu.make_async_copy(w_out.at[wrows(k, h)], wring.at[0, i], ld_sem.at[2 + i])
                   for i, h in enumerate(halves)]
            for cp in cps:
                cp.start()
            for i, h in enumerate(halves):
                cps[i].wait()

                @pl.loop(0, sw // EW)
                def _(e):
                    rows = pl.ds(mult((k * 2 + h) * sw + e * EW, EW), EW)
                    wb[0, rows, :] = wring[0, i, pl.ds(mult(e * EW, EW), EW), :].astype(BF)

        def have(i, delta, halves):
            @pl.when(jnp.logical_not(last))
            def _():
                wag[0].got_pair(i)

            @pl.when(last)
            def _():
                wfin[0].got_pair(i)
                fetch(delta, halves)

        have(0, 0, (1 - c,))
        wag[1].got_pair(0)
        for g in range(2):
            chunk(g, 0, True)
        wsum.step(1)

        @pl.when(jnp.logical_not(last))
        def _():
            got_near(wag)

        @pl.when(last)
        def _():
            got_near([wfin[0], wag[1]])

        for i, delta in ((2, -d), (1, d)):
            have(i, delta, (0, 1))
            wag[1].got_pair(i)
            for g in range(2):
                chunk(g, delta, False)

        @pl.when(jnp.logical_not(last))
        def _():
            got_far(wag)

        @pl.when(last)
        def _():
            got_far([wfin[0], wag[1]])

        @pl.when(last)
        def _():
            fetch(2, (c,))

        def far_half(g, h):
            h_part(g, (mod(wpos[g] + 2) * 2 + h) * sw, k0[g], hst, False, sw)

        for g in range(2):
            far_half(g, c)
        have(3, 2, (1 - c,))
        wag[1].got_pair(3)
        for g in range(2):
            far_half(g, 1 - c)
            for i in range(SUBS):
                h_ring(g, 0, i, True).start()
        wag[1].sent()

        @pl.when(jnp.logical_not(last))
        def _():
            wag[0].sent()

        wsum.step(2)

        @pl.loop(1, RING)
        def _(s):
            for g in range(2):
                k = mod(hpos[g] - (1 + s) * d)
                h_part(g, 0, k, hacc, True)

                @pl.loop(1, docs // BLK)
                def _(b):
                    h_part(g, b * BLK, k, hacc, False)

            @pl.when(s < RING - 1)
            def _():
                for i in range(SUBS):
                    for g in range(2):
                        h_ring(g, s - 1, i, True).wait_recv()

                        @pl.loop(0, n // EW)
                        def _(b):
                            rows = pl.ds(mult(i * n + b * EW, EW), EW)
                            hring[g, s - 1, rows, :] = hring[g, s - 1, rows, :] + hacc[g, rows, :]
                        h_ring(g, s, i, False).start()

        @pl.when(t == SWEEPS - 1)
        def _():
            for j in range(SUBS):
                wfin[1].start(j)
            for g in range(2):
                wlocal(g).start()

        wsum.step(3)
        s = RING - 1
        tot = jnp.zeros((8, topics), F32)
        for i in range(SUBS):
            for g in range(2):
                h_ring(g, s - 1, i, False).wait_recv()

            def body(b, tot):
                r0 = mult(i * n + b * 16, 16)
                rows = pl.ds(r0, 16)
                a = (hring[0, s - 1, rows, :] + hacc[0, rows, :]) + (hring[1, s - 1, rows, :] + hacc[1, rows, :])
                new = hf[rows, :] * a / jnp.concatenate([sfin[0], sfin[0]], axis=0)
                hf[rows, :] = new
                for g in range(2):
                    hb[g, pl.ds(mult(hpos[g] * sh + r0, 16), 16), :] = new.astype(BF)
                return tot + (new[:8] + new[8:])
            tot = lax.fori_loop(0, n // 16, body, tot)

            @pl.when(t < SWEEPS - 1)
            def _():
                for g in range(2):
                    hag[g].start(i)

            @pl.when(t == SWEEPS - 1)
            def _():
                hfin.start(i)

        @pl.when(t < SWEEPS - 1)
        def _():
            hsum.start(tot)

        for g in range(2):
            for ss in range(RING - 1):
                for i in range(SUBS):
                    h_ring(g, ss, i, ss == 0).wait_send()

    def wlocal(g):
        return pltpu.make_async_copy(wf.at[g], w_out.at[wrows(x, c, g * docs)], ld_sem.at[g])

    hsum.start(colsum(hf))

    @pl.loop(0, SWEEPS)
    def _(t):
        w_sweep(t)
        h_sweep(t)

    hlocal = pltpu.make_async_copy(hf, h_out.at[hrows(y)], ld_sem.at[2])
    hlocal.start()
    got_near([wfin[1], hfin])
    got_far([wfin[1], hfin])
    for g in range(2):
        if g == 1:
            for i in range(4):
                wfin[1].got_pair(i)
        wfin[g].sent()
        wlocal(g).wait()
    hfin.sent()
    hlocal.wait()


def local(c_blk, w_loc, h_loc):
    docs, words = c_blk.shape
    topics = w_loc.shape[1]
    half = docs // 2
    sw, sh = half // (2 * RING), words // RING
    dma = pltpu.SemaphoreType.DMA
    w_out, h_out = pl.pallas_call(
        kernel,
        out_shape=(jax.ShapeDtypeStruct((docs, topics), F32), jax.ShapeDtypeStruct((words, topics), F32)),
        in_specs=[pl.BlockSpec(memory_space=pl.ANY)] * 3,
        out_specs=(pl.BlockSpec(memory_space=pl.ANY), pl.BlockSpec(memory_space=pl.ANY)),
        scratch_shapes=[
            pltpu.VMEM((2, half, words), BF),
            pltpu.VMEM((2, half, topics), BF),
            pltpu.VMEM((2, words, topics), BF),
            pltpu.VMEM((2, sw, topics), F32),
            pltpu.VMEM((sh, topics), F32),
            pltpu.VMEM((2, 2 * sw, topics), F32),
            pltpu.VMEM((2, sh, topics), F32),
            pltpu.VMEM((2, RING - 1, sw, topics), F32),
            pltpu.VMEM((2, RING - 1, sh, topics), F32),
            pltpu.VMEM((2, sw, topics), F32),
            pltpu.VMEM((2, sh, topics), F32),
            pltpu.VMEM((2, 2, sw, topics), F32),
            pltpu.VMEM((2, 3, 8, topics), F32),
            pltpu.VMEM((2, 2 * RING - 1, 8, topics), F32),
            pltpu.VMEM((2, 8, topics), F32),
            dma((13,)),
            dma((RING, RING)), dma((RING, RING)),
            dma((2, RING - 1, SUBS)), dma((2, RING - 1, SUBS)),
            dma((2, RING - 1, SUBS)), dma((2, RING - 1, SUBS)),
            dma((2, 2, SUBS)), dma((2, 2, SUBS)),
            dma((7, 3, SUBS)), dma((7, 3, SUBS)),
            dma((7, 4, SUBS)), dma((7, 4, SUBS)),
            dma((2, 2 * RING - 1)), dma((2, 2 * RING - 1)),
        ],
        compiler_params=pltpu.CompilerParams(collective_id=0, has_side_effects=True,
                                             vmem_limit_bytes=63 * 1024 * 1024),
    )(c_blk, w_loc, h_loc)
    return w_out, h_out.T


def solution(mesh):
    spec_c = P(('part', 'row'), 'col')
    spec_w = P(('part', 'row'), None)
    spec_h = P(None, ('part', 'col'))
    return jax.shard_map(local, mesh=mesh, in_specs=(spec_c, spec_w, spec_h), out_specs=(spec_w, spec_h), check_vma=False)
```
